16 devices in a mesh: batch: 2 (over y, z), dap: 8 (over x, core).
Axes of the slice: x: 4, y: 2, z: 1, core: 2. Of those that a mesh axis runs over, the one named last changes fastest.
The devices are a block of a 4x4x8 slice.
Arguments:
- pair: bfloat16 [1024, 512, 64], P(('batch', 'dap')), parts along dimension 0
- pair_mask: int32 [1024, 512], P(('batch', 'dap')), parts along dimension 0
- ln_in: bfloat16 [2, 2, 64], replicated
- w_proj: bfloat16 [2, 64, 256], replicated
- b_proj: bfloat16 [2, 256], replicated
- w_gate: bfloat16 [2, 64, 64], replicated
- b_gate: bfloat16 [2, 64], replicated
- ln_out: bfloat16 [2, 2, 64], replicated
- w_out: bfloat16 [2, 64, 64], replicated
- b_out: bfloat16 [2, 64], replicated
Outputs:
- output: bfloat16 [1024, 512, 64], P(('batch', 'dap')), parts along dimension 0
There are 2 independent parts. The reference program is written for one: setup_inputs(seed, part) draws one part's arguments, and reference() takes and returns one part's arrays. A program takes and returns all parts, laid end to end along the dimension named above; an argument that names none is the same for every part.
All inputs are finite; a program needn't handle non-finite values.
Results may differ from the reference program's by a relative error of at most 0.00360069.
Values are sent between devices in bfloat16 or wider.
A program may use at most 768 MiB of HBM per device.

```python
import jax
import jax.numpy as jnp
from jax import lax

N = 512
CZ = 64
CH = 64
LN_EPS = 1e-5


def setup_inputs(seed: int = 0, part: int = 0) -> dict:
    base_key = jax.random.key(seed)
    part_key = jax.random.fold_in(base_key, part)
    pair_key, mask_key = jax.random.split(part_key)
    weight_keys = jax.random.split(jax.random.fold_in(base_key, 1000), 10)
    pair = jax.random.normal(pair_key, (N, N, CZ), jnp.float32)
    pair_mask = (jax.random.randint(mask_key, (N, N), 0, 8) > 0).astype(jnp.int32)
    ln_in = jnp.stack([1.0 + 0.3 * jax.random.normal(weight_keys[0], (2, CZ), jnp.float32),
                       0.3 * jax.random.normal(weight_keys[1], (2, CZ), jnp.float32)], axis=1)
    w_proj = jax.random.normal(weight_keys[2], (2, CZ, 4 * CH), jnp.float32) * CZ ** -0.5
    b_proj = 0.5 * jax.random.normal(weight_keys[3], (2, 4 * CH), jnp.float32)
    w_gate = jax.random.normal(weight_keys[4], (2, CZ, CZ), jnp.float32) * CZ ** -0.5
    b_gate = 0.5 * jax.random.normal(weight_keys[5], (2, CZ), jnp.float32)
    ln_out = jnp.stack([1.0 + 0.3 * jax.random.normal(weight_keys[6], (2, CH), jnp.float32),
                        0.3 * jax.random.normal(weight_keys[7], (2, CH), jnp.float32)], axis=1)
    w_out = jax.random.normal(weight_keys[8], (2, CH, CZ), jnp.float32) * CH ** -0.5
    b_out = 0.5 * jax.random.normal(weight_keys[9], (2, CZ), jnp.float32)
    return {
        "pair": pair.astype(jnp.bfloat16),
        "pair_mask": pair_mask,
        "ln_in": ln_in.astype(jnp.bfloat16),
        "w_proj": w_proj.astype(jnp.bfloat16),
        "b_proj": b_proj.astype(jnp.bfloat16),
        "w_gate": w_gate.astype(jnp.bfloat16),
        "b_gate": b_gate.astype(jnp.bfloat16),
        "ln_out": ln_out.astype(jnp.bfloat16),
        "w_out": w_out.astype(jnp.bfloat16),
        "b_out": b_out.astype(jnp.bfloat16),
    }


def layer_norm(values, scale, offset):
    centred = values - jnp.mean(values, axis=-1, keepdims=True)
    variance = jnp.mean(centred * centred, axis=-1, keepdims=True)
    return centred * lax.rsqrt(variance + LN_EPS) * scale.astype(jnp.float32) + offset.astype(jnp.float32)


def channel_product(left, right, contract_form):
    groups = CH // 16
    left_groups = jnp.moveaxis(left.reshape(N, N, groups, 16), 2, 0)
    right_groups = jnp.moveaxis(right.reshape(N, N, groups, 16), 2, 0)

    def group_sum(operands):
        return jnp.einsum(contract_form, operands[0].astype(jnp.float32), operands[1].astype(jnp.float32))

    summed = lax.map(group_sum, (left_groups, right_groups))
    return jnp.moveaxis(summed, 0, 2).reshape(N, N, CH)


def tri_layer(pair, keep_mask, ln_in, w_proj, b_proj, w_gate, b_gate, ln_out, w_out, b_out, contract_form):
    row_blocks = N // 8

    def make_sides(operands):
        block, mask_block = operands
        normed = layer_norm(block.astype(jnp.float32), ln_in[0], ln_in[1]).astype(jnp.bfloat16)
        projected = jnp.dot(normed.reshape(8 * N, CZ), w_proj, preferred_element_type=jnp.float32)
        projected = (projected + b_proj.astype(jnp.float32)).reshape(8, N, 4 * CH)
        left = mask_block * jax.nn.sigmoid(projected[..., CH:2 * CH]) * projected[..., :CH]
        right = mask_block * jax.nn.sigmoid(projected[..., 3 * CH:]) * projected[..., 2 * CH:3 * CH]
        return normed, left.astype(jnp.bfloat16), right.astype(jnp.bfloat16)

    pair_blocks = pair.reshape(row_blocks, 8, N, CZ)
    normed, left, right = lax.map(make_sides, (pair_blocks, keep_mask.reshape(row_blocks, 8, N, 1)))
    tri_sum = channel_product(left.reshape(N, N, CH), right.reshape(N, N, CH), contract_form)

    def finish(operands):
        block, normed_block, tri_block = operands
        tri_norm = layer_norm(tri_block, ln_out[0], ln_out[1]).astype(jnp.bfloat16)
        update = jnp.dot(tri_norm.reshape(8 * N, CH), w_out, preferred_element_type=jnp.float32) + b_out.astype(jnp.float32)
        gates = jax.nn.sigmoid(jnp.dot(normed_block.reshape(8 * N, CZ), w_gate, preferred_element_type=jnp.float32) + b_gate.astype(jnp.float32))
        return (block.astype(jnp.float32) + (gates * update).reshape(8, N, CZ)).astype(jnp.bfloat16)

    result = lax.map(finish, (pair_blocks, normed, tri_sum.reshape(row_blocks, 8, N, CH)))
    return result.reshape(N, N, CZ)


def reference(pair, pair_mask, ln_in, w_proj, b_proj, w_gate, b_gate, ln_out, w_out, b_out):
    keep_mask = pair_mask.astype(jnp.float32)[..., None]
    first = tri_layer(pair, keep_mask, ln_in[0], w_proj[0], b_proj[0], w_gate[0], b_gate[0],
                      ln_out[0], w_out[0], b_out[0], "ikc,jkc->ijc")
    return tri_layer(first, keep_mask, ln_in[1], w_proj[1], b_proj[1], w_gate[1], b_gate[1],
                     ln_out[1], w_out[1], b_out[1], "kic,kjc->ijc")
```

```python
import functools

import jax
import jax.numpy as jnp
from jax import lax
from jax.experimental import pallas as pl
from jax.experimental.pallas import tpu as pltpu
from jax.sharding import PartitionSpec as P

LN_EPS = 1e-5
F32 = jnp.float32
BF16 = jnp.bfloat16
VMEM_LIMIT = 60 * 1024 * 1024
LANES = 256


def cost(flops, nbytes):
    return pl.CostEstimate(flops=flops, bytes_accessed=nbytes, transcendentals=0)


def norm_rows(x, scale, offset):
    inv = 1.0 / x.shape[0]
    centred = x - jnp.sum(x, axis=0, keepdims=True) * inv
    variance = jnp.sum(centred * centred, axis=0, keepdims=True) * inv
    return centred * lax.rsqrt(variance + LN_EPS) * scale + offset


def gated_pair(low, high, w_ref, bias_ref, side):
    def half(zn, order):
        value = jnp.dot(w_ref[order, 2 * side], zn, preferred_element_type=F32)
        gate = jnp.dot(w_ref[order, 2 * side + 1], zn, preferred_element_type=F32)
        reps = zn.shape[1] // 128
        value = value + jnp.concatenate([bias_ref[order, 2 * side]] * reps, axis=1)
        gate = gate + jnp.concatenate([bias_ref[order, 2 * side + 1]] * reps, axis=1)
        out = (jnp.tanh(gate) + 1.0) * value
        return out.reshape(out.shape[0] // 8, 8, out.shape[1])

    first = half(low, 0)
    second = half(high, 1)
    upper = lax.broadcasted_iota(jnp.int32, first.shape, 1) < 4
    return jnp.where(upper, first, second), jnp.where(upper, second, first)


def sides_kernel(g, info, z_ref, m_ref, w_ref, bias_ref, ln_ref, *rest):
    a_ref, b_ref, zn_ref, zh_ref, scr = rest[-5:]
    dev = pl.program_id(0)
    mine = lax.rem(dev, 2) == info[1]
    rows, chans, cols = scr.shape

    for r in range(rows):
        for l in range(0, cols, LANES):
            x = z_ref[0, r, :, l:l + LANES].astype(F32)
            scr[r, :, l:l + LANES] = norm_rows(x, ln_ref[0], ln_ref[1]).astype(BF16)

    def emit(out_ref, side):
        for l in range(0, cols, LANES):
            even, odd = [], []
            for h in range(0, rows, 8):
                low = scr[h:h + 4, :, l:l + LANES].reshape(4 * chans, LANES)
                high = scr[h + 4:h + 8, :, l:l + LANES].reshape(4 * chans, LANES)
                e, o = gated_pair(low, high, w_ref, bias_ref, side)
                mask = m_ref[h:h + 8, l:l + LANES].astype(F32)
                even.append(e * mask[None])
                odd.append(pltpu.roll(o, 4, 1) * mask[None])
            out_ref[:, 0, :, l:l + LANES] = jnp.concatenate(even, axis=1).astype(BF16)
            out_ref[:, 1, :, l:l + LANES] = jnp.concatenate(odd, axis=1).astype(BF16)

    emit(b_ref, 1)

    @pl.when(mine)
    def _():
        emit(a_ref, 0)
        zn_ref[...] = scr[...]
        zh_ref[...] = z_ref[0]


def sides_call(g, chunks, info, zg, mask, w4, bias4, ln, prev):
    devs, rows, chans, cols = zg.shape
    per = chunks
    shapes = [jax.ShapeDtypeStruct((chans // 2, 2, devs // 2 * per * rows, cols), BF16),
              jax.ShapeDtypeStruct((chans // 2, 2, devs * per * rows, cols), BF16),
              jax.ShapeDtypeStruct((devs // 2 * per * rows, chans, cols), BF16),
              jax.ShapeDtypeStruct((devs // 2 * per * rows, chans, cols), BF16)]
    full = lambda arr: pl.BlockSpec(arr.shape, lambda i, info: (0,) * arr.ndim)
    in_specs = [pl.BlockSpec((1, rows, chans, cols), lambda i, info: (i, 0, 0, 0)),
                pl.BlockSpec((rows, cols), lambda i, info: (i * per + g, 0)),
                full(w4), full(bias4), full(ln)]
    args = [zg, mask, w4, bias4, ln]
    aliases = {}
    if prev is not None:
        in_specs += [pl.BlockSpec(memory_space=pl.ANY)] * 4
        aliases = {1 + len(args) + n: n for n in range(4)}
        args += list(prev)
    half_row = lambda i, info: (lax.div(i, 2) * per + g, 0, 0)
    out_specs = [pl.BlockSpec((chans // 2, 2, rows, cols), lambda i, info: (0, 0, lax.div(i, 2) * per + g, 0)),
                 pl.BlockSpec((chans // 2, 2, rows, cols), lambda i, info: (0, 0, i * per + g, 0)),
                 pl.BlockSpec((rows, chans, cols), half_row),
                 pl.BlockSpec((rows, chans, cols), half_row)]
    return pl.pallas_call(
        functools.partial(sides_kernel, g),
        out_shape=shapes,
        grid_spec=pltpu.PrefetchScalarGridSpec(
            num_scalar_prefetch=1, grid=(devs,), in_specs=in_specs, out_specs=out_specs,
            scratch_shapes=[pltpu.VMEM((rows, chans, cols), BF16)]),
        input_output_aliases=aliases,
        compiler_params=pltpu.CompilerParams(vmem_limit_bytes=VMEM_LIMIT, dimension_semantics=("arbitrary",)),
        cost_estimate=cost(12_000_000_000, 40_000_000),
        name=f"sides_{g}",
    )(info, *args)


def finish_rows(v, zn, z, ln_ref, wo_ref, bo_ref, wg_ref, bg_ref):
    chans, rows, n = v.shape
    inv = 1.0 / chans
    reps = n // 128
    wide = lambda ref, k: jnp.concatenate([ref[k]] * reps, axis=-1)
    mean = jnp.sum(v, axis=0) * inv
    centred = v - mean[None]
    variance = jnp.sum(centred * centred, axis=0) * inv
    normed = centred * lax.rsqrt(variance + LN_EPS)[None]
    normed = normed * wide(ln_ref, 0) + wide(ln_ref, 1)
    u = normed.reshape(chans * rows, n).astype(BF16)
    update = jnp.dot(wo_ref[...], u, preferred_element_type=F32) + jnp.concatenate([bo_ref[...]] * reps, axis=1)
    k = wg_ref.shape[0]
    zn2 = zn.reshape(rows * chans, n)
    gate = jnp.concatenate([jnp.dot(wg_ref[...], zn2[q:q + k], preferred_element_type=F32)
                            for q in range(0, rows * chans, k)], axis=0)
    gate = jnp.tanh(gate + jnp.concatenate([bg_ref[...]] * reps, axis=1)) + 1.0
    out = z.astype(F32).reshape(rows * chans, n) + gate * update
    return out.astype(BF16).reshape(rows, chans, n)


def first_kernel(a_ref, b_ref, zn_ref, z_ref, ln_ref, wo_ref, bo_ref, wg_ref, bg_ref, out_ref, o_scr):
    t, s = pl.program_id(0), pl.program_id(1)
    per = a_ref.shape[0]

    @pl.when(t < 2)
    def _():
        for q in range(per):
            o_scr[lax.rem(t, 2), s * per + q] = lax.dot_general(
                a_ref[q], b_ref[q], (((1,), (1,)), ((), ())), preferred_element_type=F32)

    @pl.when(t > 0)
    def _():
        rows = out_ref.shape[0]

        @pl.loop(0, rows, step=8)
        def _(r):
            start = pl.multiple_of(s * rows + r, 8)
            v = o_scr[lax.rem(t + 1, 2), :, pl.ds(start, 8), :]
            out_ref[pl.ds(r, 8)] = finish_rows(v, zn_ref[pl.ds(r, 8)], z_ref[pl.ds(r, 8)],
                                               ln_ref, wo_ref, bo_ref, wg_ref, bg_ref)


def first_call(a, b, zn, zh, fin):
    chans, rows, cols = a.shape
    steps = 8
    per = chans // steps
    tile = LANES
    ntile = b.shape[1] // tile
    assert ntile == 2
    rstep = rows // steps
    full = lambda arr: pl.BlockSpec(arr.shape, lambda t, s: (0,) * arr.ndim)
    last = steps - 1
    row_map = lambda t, s: (jnp.where(t > 0, s, 0), 0, jnp.maximum(t - 1, 0))
    return pl.pallas_call(
        first_kernel,
        out_shape=jax.ShapeDtypeStruct(zh.shape, BF16),
        grid=(ntile + 1, steps),
        in_specs=[pl.BlockSpec((per, rows, cols), lambda t, s: (jnp.where(t < 2, s, last), 0, 0)),
                  pl.BlockSpec((per, tile, cols), lambda t, s: (jnp.where(t < 2, s, last), jnp.minimum(t, 1), 0)),
                  pl.BlockSpec((rstep, zn.shape[1], tile), row_map),
                  pl.BlockSpec((rstep, zn.shape[1], tile), row_map)] + [full(f) for f in fin],
        out_specs=pl.BlockSpec((rstep, zn.shape[1], tile), row_map),
        scratch_shapes=[pltpu.VMEM((2, chans, rows, tile), F32)],
        compiler_params=pltpu.CompilerParams(vmem_limit_bytes=VMEM_LIMIT,
                                             dimension_semantics=("arbitrary", "arbitrary")),
        cost_estimate=cost(40_000_000_000, 140_000_000),
        name="first_layer",
    )(a, b, zn, zh, *fin)


def second_sides_kernel(info, z_ref, m_ref, w_ref, bias_ref, ln_ref, a_ref, b_ref, scr):
    rows, chans, cols = scr.shape
    for r in range(rows):
        for l in range(0, cols, LANES):
            x = z_ref[r, :, l:l + LANES].astype(F32)
            scr[r, :, l:l + LANES] = norm_rows(x, ln_ref[0], ln_ref[1]).astype(BF16)

    def emit(out_ref, side, width, start, out_start):
        even, odd = [], []
        for h in range(0, rows, 8):
            low = scr[h:h + 4, :, pl.ds(start, width)].reshape(4 * chans, width)
            high = scr[h + 4:h + 8, :, pl.ds(start, width)].reshape(4 * chans, width)
            e, o = gated_pair(low, high, w_ref, bias_ref, side)
            mask = m_ref[h:h + 8, pl.ds(start, width)].astype(F32)
            even.append(e * mask[None])
            odd.append(o * pltpu.roll(mask, 4, 0)[None])
        out_ref[:, 0, :, out_start:out_start + width] = jnp.concatenate(even, axis=1).astype(BF16)
        out_ref[:, 1, :, out_start:out_start + width] = jnp.concatenate(odd, axis=1).astype(BF16)

    for l in range(0, cols, LANES):
        emit(b_ref, 1, LANES, l, l)
    width = a_ref.shape[3]
    emit(a_ref, 0, width, pl.multiple_of(info[0] * width, width), 0)


def second_sides_call(info, z1, mask, w4, bias4, ln, width, per):
    nrow, chans, cols = z1.shape
    rows = 16
    full = lambda arr: pl.BlockSpec(arr.shape, lambda i, info: (0,) * arr.ndim)
    mask_map = lambda i, info: ((2 * lax.div(i, per) + info[1]) * per + lax.rem(i, per), 0)
    return pl.pallas_call(
        second_sides_kernel,
        out_shape=[jax.ShapeDtypeStruct((chans // 2, 2, nrow, width), BF16),
                   jax.ShapeDtypeStruct((chans // 2, 2, nrow, cols), BF16)],
        grid_spec=pltpu.PrefetchScalarGridSpec(
            num_scalar_prefetch=1, grid=(nrow // rows,),
            in_specs=[pl.BlockSpec((rows, chans, cols), lambda i, info: (i, 0, 0)),
                      pl.BlockSpec((rows, cols), mask_map), full(w4), full(bias4), full(ln)],
            out_specs=[pl.BlockSpec((chans // 2, 2, rows, width), lambda i, info: (0, 0, i, 0)),
                       pl.BlockSpec((chans // 2, 2, rows, cols), lambda i, info: (0, 0, i, 0))],
            scratch_shapes=[pltpu.VMEM((rows, chans, cols), BF16)]),
        compiler_params=pltpu.CompilerParams(vmem_limit_bytes=VMEM_LIMIT, dimension_semantics=("arbitrary",)),
        cost_estimate=cost(12_000_000_000, 40_000_000),
        name="second_sides",
    )(info, z1, mask, w4, bias4, ln)


def partial_kernel(info, a_ref, b_ref, keep_ref, send_ref):
    half = keep_ref.shape[1]

    def run(own, other):
        for q in range(a_ref.shape[0]):
            total = lax.dot_general(a_ref[q], b_ref[q], (((0,), (0,)), ((), ())), preferred_element_type=F32)
            own[q] = total[:half]
            other[q] = total[half:]

    @pl.when(info[1] == 0)
    def _():
        run(keep_ref, send_ref)

    @pl.when(info[1] == 1)
    def _():
        run(send_ref, keep_ref)


def partial_call(info, a, b, part, parts):
    chans, rows, width = a.shape
    cols = b.shape[2] // parts
    per = 8
    out = jax.ShapeDtypeStruct((chans, width // 2, cols), F32)
    return pl.pallas_call(
        partial_kernel,
        out_shape=[out, out],
        grid_spec=pltpu.PrefetchScalarGridSpec(
            num_scalar_prefetch=1, grid=(chans // per,),
            in_specs=[pl.BlockSpec((per, rows, width), lambda i, info: (i, 0, 0)),
                      pl.BlockSpec((per, rows, cols), lambda i, info: (i, 0, part))],
            out_specs=[pl.BlockSpec((per, width // 2, cols), lambda i, info: (i, 0, 0))] * 2),
        compiler_params=pltpu.CompilerParams(vmem_limit_bytes=VMEM_LIMIT, dimension_semantics=("arbitrary",)),
        cost_estimate=cost(5_000_000_000, 20_000_000),
        name=f"partial_{part}",
    )(info, a, b)


def second_kernel(info, own_ref, got_ref, z_ref, lni_ref, ln_ref, wo_ref, bo_ref, wg_ref, bg_ref, *rest):
    out_ref, scr = rest[-2:]
    rows, chans, n = scr.shape
    for r in range(rows):
        scr[r] = norm_rows(z_ref[r].astype(F32), lni_ref[0], lni_ref[1]).astype(BF16)
    for r in range(0, rows, 8):
        v = own_ref[:, r:r + 8, :] + got_ref[:, r:r + 8, :]
        out_ref[r:r + 8] = finish_rows(v, scr[r:r + 8], z_ref[r:r + 8], ln_ref, wo_ref, bo_ref, wg_ref, bg_ref)


def second_call(info, own, got, z1, lni, fin, part, prev):
    chans, nrow, n = own.shape
    rows = 16
    full = lambda arr: pl.BlockSpec(arr.shape, lambda i, info: (0,) * arr.ndim)
    steps = nrow // rows
    args = [own, got, z1, lni] + list(fin)
    in_specs = [pl.BlockSpec((chans, rows, n), lambda i, info: (0, i, 0)),
                pl.BlockSpec((chans, rows, n), lambda i, info: (0, i, 0)),
                pl.BlockSpec((rows, chans, n), lambda i, info: (info[0] * steps + i, 0, part)),
                full(lni)] + [full(f) for f in fin]
    aliases = {}
    if prev is not None:
        aliases = {1 + len(args): 0}
        args.append(prev)
        in_specs.append(pl.BlockSpec(memory_space=pl.ANY))
    return pl.pallas_call(
        second_kernel,
        out_shape=jax.ShapeDtypeStruct((nrow, chans, z1.shape[2]), BF16),
        grid_spec=pltpu.PrefetchScalarGridSpec(
            num_scalar_prefetch=1, grid=(steps,), in_specs=in_specs,
            out_specs=pl.BlockSpec((rows, chans, n), lambda i, info: (i, 0, part)),
            scratch_shapes=[pltpu.VMEM((rows, chans, n), BF16)]),
        input_output_aliases=aliases,
        compiler_params=pltpu.CompilerParams(vmem_limit_bytes=VMEM_LIMIT, dimension_semantics=("arbitrary",)),
        cost_estimate=cost(5_000_000_000, 20_000_000),
        name=f"second_layer_{part}",
    )(info, *args)


def side_weights(w_proj, b_proj, chans):
    wt = (0.5 * w_proj.astype(F32)).T.reshape(4, chans, -1)
    bias = (0.5 * b_proj.astype(F32)).reshape(4, chans)
    swap = lambda x: x.reshape((4, chans // 2, 2) + x.shape[2:])[:, :, ::-1].reshape(x.shape)
    eye = jnp.eye(4, dtype=F32)
    spread = lambda x: (x[:, :, None, None, :] * eye[None, None, :, :, None]).reshape(4, 4 * chans, -1)
    w4 = jnp.stack([spread(wt), spread(swap(wt))]).astype(BF16)
    rep = lambda x: jnp.broadcast_to(x[:, :, None, None], (4, chans, 4, 128)).reshape(4, 4 * chans, 128)
    return w4, jnp.stack([rep(bias), rep(swap(bias))])


def finish_weights(ln_out, w_out, b_out, w_gate, b_gate):
    chans = w_out.shape[0]
    ln = jnp.broadcast_to(ln_out.astype(F32)[:, :, None, None], (2, chans, 8, 128))
    eye8 = jnp.eye(8, dtype=F32)
    wo = 0.5 * w_out.astype(F32)
    wo = (wo.T[None, :, :, None] * eye8[:, None, None, :]).reshape(8 * wo.shape[1], chans * 8).astype(BF16)
    bo = jnp.broadcast_to((0.5 * b_out.astype(F32))[None, :, None], (8, chans, 128)).reshape(8 * chans, 128)
    eye4 = jnp.eye(4, dtype=F32)
    wg = 0.5 * w_gate.astype(F32)
    wg = (wg.T[None, :, None, :] * eye4[:, None, :, None]).reshape(4 * chans, 4 * chans).astype(BF16)
    bg = jnp.broadcast_to((0.5 * b_gate.astype(F32))[None, :, None], (8, chans, 128)).reshape(8 * chans, 128)
    return ln, wo, bo, wg, bg


def in_norm(ln_in, width):
    return jnp.broadcast_to(ln_in.astype(F32)[:, :, None], (2, ln_in.shape[1], width))


def solution(mesh):
    row_spec = P(("batch", "dap"), None, None)
    mask_spec = P(("batch", "dap"), None)
    devs = mesh.shape["dap"]

    def local_layers(pair, pair_mask, ln_in, w_proj, b_proj, w_gate, b_gate, ln_out, w_out, b_out):
        nrow, cols, chans = pair.shape
        me = lax.axis_index("dap")
        info = jnp.stack([lax.div(me, 2), lax.rem(me, 2)]).astype(jnp.int32)
        zt = pair.transpose(0, 2, 1)
        rows = 16
        chunks = nrow // rows
        mask = lax.all_gather(pair_mask, "dap", axis=0, tiled=True)
        w4, bias4 = side_weights(w_proj[0], b_proj[0], chans)
        w4b, bias4b = side_weights(w_proj[1], b_proj[1], chans)
        lni = in_norm(ln_in[0], LANES)
        lnib = in_norm(ln_in[1], LANES)
        fin = finish_weights(ln_out[0], w_out[0], b_out[0], w_gate[0], b_gate[0])
        finb = finish_weights(ln_out[1], w_out[1], b_out[1], w_gate[1], b_gate[1])
        parts = None
        for g in range(chunks):
            zg = lax.all_gather(zt[g * rows:(g + 1) * rows], "dap", axis=0, tiled=False)
            parts = sides_call(g, chunks, info, zg, mask, w4, bias4, lni, parts)
        a, b, zn, zh = parts
        merge = lambda x: x.reshape((chans,) + x.shape[2:])
        z1 = first_call(merge(a), merge(b), zn, zh, fin)
        width = 2 * nrow
        a2, b2 = second_sides_call(info, z1, mask, w4b, bias4b, lnib, width, chunks)
        a2, b2 = merge(a2), merge(b2)
        pairs = [(d, d + 1 - 2 * (d % 2)) for d in range(devs)]
        out = None
        nparts = cols // LANES
        sums = []
        for p in range(nparts):
            own, send = partial_call(info, a2, b2, p, nparts)
            sums.append((own, lax.ppermute(send, "dap", pairs)))
        for p, (own, got) in enumerate(sums):
            out = second_call(info, own, got, z1, lnib, finb, p, out)
        return out.transpose(0, 2, 1)

    return jax.shard_map(local_layers, mesh=mesh,
                         in_specs=(row_spec, mask_spec, P(), P(), P(), P(), P(), P(), P(), P()),
                         out_specs=row_spec, check_vma=False)
```
